32 devices in a mesh: path: 16 (over z, x, core), shard: 2 (over y).
Axes of the slice: x: 2, y: 2, z: 4, core: 2. Of those that a mesh axis runs over, the one named last changes fastest.
Arguments:
- deltas: bfloat16 [16, 32, 4096], P('path', 'shard'), may hold values from -96 to 96
- momentum: float32 [16, 32, 4096], P(None, 'shard', 'path'), may hold values from -4 to 4
- path_module: int32 [16], replicated, may hold values from 0 to 15, as said below
Outputs:
- path_update: bfloat16 [16, 32, 4096], P('path', 'shard')
- new_momentum: float32 [16, 32, 4096], P(None, 'shard', 'path')
The draws below stay inside these ranges and needn't reach their ends.
Inputs may be any that keep to these rules, and one draw needn't show every extreme that they name: `path_module`: every module is used by at least one and at most seven paths.
All inputs are finite; a program needn't handle non-finite values.
Results may differ from the reference program's by a relative error of at most 0.0004.
Values may be sent and summed in bfloat16 or wider, within the bound.
A program may use at most 64 MiB of HBM per device.

```python
import jax
import jax.numpy as jnp
from jax import lax

D = 4096
MODULES = 16
ROWS = 32
PATHS = 16


def draw_deltas(key, part):
    row_pos = jnp.arange(ROWS, dtype=jnp.float32) / ROWS
    col_pos = jnp.arange(D, dtype=jnp.float32) / D
    ramp = (1.0 + row_pos)[:, None] * (1.0 + col_pos)[None, :]
    log_scale = jax.random.uniform(jax.random.fold_in(key, 7), (PATHS, 1, 1), jnp.float32, -1.3862944, 1.3862944)
    path_scale = jnp.exp(log_scale)
    values = jnp.clip(jax.random.normal(key, (PATHS, ROWS, D), jnp.float32), -6.0, 6.0) * path_scale
    return (values * ramp).astype(jnp.bfloat16)


def draw_path_module(key, part):
    first = jax.random.permutation(jax.random.fold_in(key, 1), MODULES).astype(jnp.int32)
    repeated = jnp.tile(jnp.arange(MODULES, dtype=jnp.int32), 6)
    others = jax.random.permutation(jax.random.fold_in(key, 2), repeated)[:PATHS - MODULES].astype(jnp.int32)
    labels = jnp.concatenate([first, others])
    return jax.random.permutation(jax.random.fold_in(key, 3), labels).astype(jnp.int32)


def shard_levels(stream_key, dims, cuts, low, largest):
    factor_of, own = 1.0, jax.random.fold_in(stream_key, 6)
    for axis_at, shards_of in cuts:
        steps = jnp.exp(jax.random.uniform(jax.random.fold_in(own, axis_at), (shards_of,), jnp.float32, low / len(cuts), largest / len(cuts)))
        factor_of = factor_of * jnp.repeat(steps, dims[axis_at] // shards_of).reshape([-1 if axis == axis_at else 1 for axis in range(len(dims))])
    return factor_of


def normal_values(rng, extent, deviation, bound, pieces=(), kind=jnp.bfloat16):
    entries = jax.random.normal(rng, extent, jnp.float32) * deviation
    if len(pieces) > 0:
        entries = shard_levels(rng, extent, pieces, -0.22, 0.18) * entries
    return jnp.clip(entries, min=-bound, max=bound).astype(kind)


def setup_inputs(seed: int = 0) -> dict:
    keys = jax.random.split(jax.random.key(seed), 4)
    deltas = draw_deltas(jax.random.fold_in(keys[3], 71), 0)
    momentum = normal_values(keys[1], (MODULES, ROWS, D), 0.25, 4.0, ((1, 2), (2, 16)), jnp.float32)
    path_module = draw_path_module(jax.random.fold_in(keys[3], 71), 0)
    return dict(deltas=deltas, momentum=momentum, path_module=path_module)


outer_rate = 0.7
momentum_rate = 0.9
clip_ratio = 2.0

def reference(deltas, momentum, path_module):
    onehot = (path_module[:, None] == jnp.arange(MODULES, dtype=jnp.int32)[None, :]).astype(jnp.float32)
    counts = lax.optimization_barrier(jnp.sum(onehot, axis=0))
    totals = jnp.einsum('pm,prc->mrc', onehot, deltas.astype(jnp.float32), precision=lax.Precision.HIGHEST)
    outer_grad = totals / counts[:, None, None]
    norm_squares = lax.optimization_barrier(jnp.sum(outer_grad * outer_grad, axis=(1, 2)))
    limit = clip_ratio * jnp.sqrt(jnp.float32(ROWS * D))
    shrink = jnp.minimum(1.0, limit / jnp.sqrt(norm_squares + 1e-06))
    clipped = outer_grad * shrink[:, None, None]
    new_momentum = momentum_rate * momentum + clipped
    outer_step = (outer_rate * (clipped + momentum_rate * new_momentum)).astype(jnp.bfloat16)
    path_update = jnp.einsum('pm,mrc->prc', onehot, outer_step.astype(jnp.float32), precision=lax.Precision.HIGHEST).astype(jnp.bfloat16)
    return (path_update, new_momentum)
```

```python
import functools
import math

import jax
import jax.numpy as jnp
from jax import lax
from jax.experimental import pallas as pl
from jax.experimental.pallas import tpu as pltpu
from jax.sharding import PartitionSpec as P

outer_rate = 0.7
momentum_rate = 0.9
clip_ratio = 2.0
LANES = 128
MESH = pl.DeviceIdType.MESH


def kernel(
    n,
    s,
    deltas_ref,
    momentum_ref,
    module_ref,
    update_ref,
    new_ref,
    own,
    pieces,
    momentum,
    grad,
    new,
    step,
    chosen,
    squares,
    load_sem,
    local_sem,
    send_sem,
    recv_sem,
    square_send,
    square_recv,
    back_send,
    back_recv,
):
    me, my_shard = lax.axis_index("path"), lax.axis_index("shard")
    modules, rows, columns = momentum.shape
    width = own.shape[1]
    everyone = [(k, j) for k in range(n) for j in range(s) if (k, j) != (0, 0)]

    def peer(k, j=0):
        return lax.rem(me + k, n), lax.rem(my_shard + j, s)

    def device(k, j=0):
        there, shard = peer(k, j)
        return {"path": there, "shard": shard}

    def block(index):
        return pl.ds(pl.multiple_of(index * columns, columns), columns)

    load_own = pltpu.make_async_copy(deltas_ref.at[0], own, load_sem.at[0])
    load_own.start()
    load_momentum = pltpu.make_async_copy(momentum_ref, momentum, load_sem.at[1])
    load_momentum.start()
    barrier = pltpu.get_barrier_semaphore()
    for k, j in everyone:
        pl.semaphore_signal(barrier, inc=1, device_id=device(k, j), device_id_type=MESH)

    lane = lax.broadcasted_iota(jnp.int32, (1, n * rows), 1)
    target = jnp.zeros((1, n * rows), jnp.int32)
    for p in range(n):
        inside = (lane >= p * rows) & (lane < (p + 1) * rows)
        target = jnp.where(inside, lane + (module_ref[p] - p) * rows, target)
    row = lax.broadcasted_iota(jnp.int32, (modules * rows, n * rows), 0)
    spread = (row == target).astype(jnp.float32)
    scale = 1.0 / jnp.sum(spread, axis=1, keepdims=True)
    spread = spread.astype(jnp.bfloat16)

    load_own.wait()
    keep_own = pltpu.make_async_copy(own.at[:, block(me)], pieces.at[me], local_sem.at[0])
    keep_own.start()
    pl.semaphore_wait(barrier, len(everyone))
    sends = []
    for k in range(1, n):
        there, _ = peer(k)
        copy = pltpu.make_async_remote_copy(
            src_ref=own.at[:, block(there)],
            dst_ref=pieces.at[me],
            send_sem=send_sem.at[k],
            recv_sem=recv_sem.at[k],
            device_id=device(k),
            device_id_type=MESH,
        )
        copy.start()
        sends.append(copy)
    keep_own.wait()
    for copy in sends:
        copy.wait_recv()

    total = jnp.dot(
        spread, pieces[...].reshape(n * rows, columns), preferred_element_type=jnp.float32
    )
    outer_grad = (total * scale).reshape(modules, rows, columns)
    grad[...] = outer_grad
    by_row = jnp.sum(outer_grad * outer_grad, axis=1)
    by_module = jnp.sum(by_row, axis=1, keepdims=True)
    on_diagonal = lax.broadcasted_iota(
        jnp.int32, (modules, LANES), 0
    ) == lax.broadcasted_iota(jnp.int32, (modules, LANES), 1)
    own_squares = jnp.sum(jnp.where(on_diagonal, by_module, 0.0), axis=0, keepdims=True)
    my_slot = me * s + my_shard
    squares[my_slot] = own_squares
    square_copies = []
    for at, (k, j) in enumerate(everyone):
        copy = pltpu.make_async_remote_copy(
            src_ref=squares.at[my_slot],
            dst_ref=squares.at[my_slot],
            send_sem=square_send.at[at],
            recv_sem=square_recv.at[at],
            device_id=device(k, j),
            device_id_type=MESH,
        )
        copy.start()
        square_copies.append(copy)
    load_momentum.wait()
    for copy in square_copies:
        copy.wait_recv()
    norm_squares = jnp.sum(squares[...], axis=0)
    limit = clip_ratio * math.sqrt(rows * s * width)
    shrink = jnp.minimum(1.0, limit / jnp.sqrt(norm_squares + 1e-06))
    at_lane = lax.broadcasted_iota(jnp.int32, (1, LANES), 1)
    for m in range(modules):
        factor = jnp.sum(jnp.where(at_lane == m, shrink, 0.0), axis=1, keepdims=True)
        clipped = grad[m] * factor
        moved = momentum_rate * momentum[m] + clipped
        new[m] = moved
        step[m] = (outer_rate * (clipped + momentum_rate * moved)).astype(jnp.bfloat16)
    for p in range(n):
        chosen[p] = step[module_ref[p]]
    returns = []
    for k in range(1, n):
        there, _ = peer(k)
        copy = pltpu.make_async_remote_copy(
            src_ref=chosen.at[there],
            dst_ref=update_ref.at[0, :, block(me)],
            send_sem=back_send.at[k],
            recv_sem=back_recv.at[k],
            device_id=device(k),
            device_id_type=MESH,
        )
        copy.start()
        returns.append(copy)
    put_own = pltpu.make_async_copy(
        chosen.at[me], update_ref.at[0, :, block(me)], local_sem.at[1]
    )
    put_own.start()
    put_new = pltpu.make_async_copy(new, new_ref, local_sem.at[2])
    put_new.start()
    for copy in sends + square_copies:
        copy.wait_send()
    put_own.wait()
    put_new.wait()
    for copy in returns:
        copy.wait()


def direct(n, s, deltas, momentum, path_module):
    modules, rows, columns = momentum.shape
    width = deltas.shape[2]
    dma = pltpu.SemaphoreType.DMA
    anywhere = pl.BlockSpec(memory_space=pl.ANY)
    return pl.pallas_call(
        functools.partial(kernel, n, s),
        out_shape=(
            jax.ShapeDtypeStruct(deltas.shape, jnp.bfloat16),
            jax.ShapeDtypeStruct(momentum.shape, jnp.float32),
        ),
        in_specs=[anywhere, anywhere, pl.BlockSpec(memory_space=pltpu.SMEM)],
        out_specs=(anywhere, anywhere),
        scratch_shapes=[
            pltpu.VMEM((rows, width), jnp.bfloat16),
            pltpu.VMEM((n, rows, columns), jnp.bfloat16),
            pltpu.VMEM((modules, rows, columns), jnp.float32),
            pltpu.VMEM((modules, rows, columns), jnp.float32),
            pltpu.VMEM((modules, rows, columns), jnp.float32),
            pltpu.VMEM((modules, rows, columns), jnp.bfloat16),
            pltpu.VMEM((n, rows, columns), jnp.bfloat16),
            pltpu.VMEM((n * s, 1, LANES), jnp.float32),
            dma((2,)),
            dma((3,)),
            dma((n,)),
            dma((n,)),
            dma((n * s,)),
            dma((n * s,)),
            dma((n,)),
            dma((n,)),
        ],
        compiler_params=pltpu.CompilerParams(collective_id=0, has_side_effects=True),
    )(deltas, momentum, path_module)


def by_collectives(s, deltas, momentum, path_module):
    modules = momentum.shape[0]
    rows, width = deltas.shape[1:]
    onehot = path_module[:, None] == jnp.arange(modules, dtype=jnp.int32)[None, :]
    counts = jnp.sum(onehot.astype(jnp.float32), axis=0)
    pieces = lax.all_to_all(deltas, "path", split_axis=2, concat_axis=0, tiled=True)
    totals = jnp.einsum(
        "pm,prc->mrc", onehot.astype(jnp.bfloat16), pieces, preferred_element_type=jnp.float32
    )
    outer_grad = totals / counts[:, None, None]
    local_squares = jnp.sum(outer_grad * outer_grad, axis=(1, 2))
    norm_squares = lax.psum(local_squares, ("path", "shard"))
    limit = clip_ratio * math.sqrt(rows * s * width)
    shrink = jnp.minimum(1.0, limit / jnp.sqrt(norm_squares + 1e-06))
    clipped = outer_grad * shrink[:, None, None]
    new_momentum = momentum_rate * momentum + clipped
    outer_step = (outer_rate * (clipped + momentum_rate * new_momentum)).astype(jnp.bfloat16)
    chosen = jnp.take(outer_step, path_module, axis=0)
    path_update = lax.all_to_all(chosen, "path", split_axis=0, concat_axis=2, tiled=True)
    return (path_update, new_momentum)


def local(n, s, deltas, momentum, path_module):
    modules, rows, columns = momentum.shape
    aligned = columns % LANES == 0 and rows % 16 == 0 and modules <= LANES
    if aligned and n > 1:
        return direct(n, s, deltas, momentum, path_module)
    return by_collectives(s, deltas, momentum, path_module)


def solution(mesh):
    return jax.shard_map(
        functools.partial(local, mesh.shape["path"], mesh.shape["shard"]),
        mesh=mesh,
        in_specs=(P("path", "shard", None), P(None, "shard", "path"), P()),
        out_specs=(P("path", "shard", None), P(None, "shard", "path")),
        check_vma=False,
    )
```

```python
import functools
import math

import jax
import jax.numpy as jnp
from jax import lax
from jax.experimental import pallas as pl
from jax.experimental.pallas import tpu as pltpu
from jax.sharding import PartitionSpec as P

outer_rate = 0.7
momentum_rate = 0.9
clip_ratio = 2.0
LANES = 128
MESH = pl.DeviceIdType.MESH


def kernel(
    n,
    s,
    deltas_ref,
    momentum_ref,
    path_module_ref,
    update,
    new,
    module_ref,
    own,
    pieces,
    momentum,
    grad,
    step,
    chosen,
    mine,
    squares,
    load_sem,
    send_sem,
    recv_sem,
    square_send,
    square_recv,
    back_send,
    back_recv,
):
    me, my_shard = lax.axis_index("path"), lax.axis_index("shard")
    modules, rows, columns = momentum.shape
    width = own.shape[1]
    everyone = [(k, j) for k in range(n) for j in range(s) if (k, j) != (0, 0)]

    def peer(k, j=0):
        return lax.rem(me + k, n), lax.rem(my_shard + j, s)

    def device(k, j=0):
        there, shard = peer(k, j)
        return {"path": there, "shard": shard}

    def arrived(buffer, sem):
        pltpu.make_async_copy(buffer, buffer, sem).wait()

    def block(index):
        return pl.ds(pl.multiple_of(index * columns, columns), columns)

    barrier = pltpu.get_barrier_semaphore()
    for k, j in everyone:
        pl.semaphore_signal(barrier, inc=1, device_id=device(k, j), device_id_type=MESH)
    load_module = pltpu.make_async_copy(path_module_ref, module_ref, load_sem.at[2])
    load_module.start()
    load_own = pltpu.make_async_copy(deltas_ref.at[0], own, load_sem.at[0])
    load_own.start()
    load_momentum = pltpu.make_async_copy(momentum_ref, momentum, load_sem.at[1])
    load_momentum.start()
    load_module.wait()

    lane = lax.broadcasted_iota(jnp.int32, (1, n * rows), 1)
    target = jnp.zeros((1, n * rows), jnp.int32)
    for p in range(n):
        inside = (lane >= p * rows) & (lane < (p + 1) * rows)
        target = jnp.where(inside, lane + (module_ref[p] - p) * rows, target)
    row = lax.broadcasted_iota(jnp.int32, (modules * rows, n * rows), 0)
    spread = (row == target).astype(jnp.float32)
    scale = 1.0 / jnp.sum(spread, axis=1, keepdims=True)
    spread = spread.astype(jnp.bfloat16)

    load_own.wait()
    keep_own = pltpu.make_async_copy(own.at[:, block(me)], pieces.at[me], recv_sem)
    keep_own.start()
    pl.semaphore_wait(barrier, len(everyone))
    for k in range(1, n):
        there, _ = peer(k)
        copy = pltpu.make_async_remote_copy(
            src_ref=own.at[:, block(there)],
            dst_ref=pieces.at[me],
            send_sem=send_sem,
            recv_sem=recv_sem,
            device_id=device(k),
            device_id_type=MESH,
        )
        copy.start()
    arrived(pieces, recv_sem)

    total = jnp.dot(
        spread, pieces[...].reshape(n * rows, columns), preferred_element_type=jnp.float32
    )
    outer_grad = (total * scale).reshape(modules, rows, columns)
    grad[...] = outer_grad
    by_row = jnp.sum(outer_grad * outer_grad, axis=1)
    by_module = jnp.sum(by_row, axis=1, keepdims=True)
    on_diagonal = lax.broadcasted_iota(
        jnp.int32, (modules, LANES), 0
    ) == lax.broadcasted_iota(jnp.int32, (modules, LANES), 1)
    own_squares = jnp.sum(jnp.where(on_diagonal, by_module, 0.0), axis=0, keepdims=True)
    my_slot = me * s + my_shard
    mine[...] = own_squares
    for k, j in everyone:
        copy = pltpu.make_async_remote_copy(
            src_ref=mine,
            dst_ref=squares.at[my_slot],
            send_sem=square_send,
            recv_sem=square_recv,
            device_id=device(k, j),
            device_id_type=MESH,
        )
        copy.start()
    pltpu.make_async_copy(mine, squares.at[my_slot], square_recv).start()
    load_momentum.wait()
    arrived(squares, square_recv)
    norm_squares = jnp.sum(squares[...], axis=0)
    limit = clip_ratio * math.sqrt(rows * s * width)
    shrink = jnp.minimum(1.0, limit / jnp.sqrt(norm_squares + 1e-06))
    at_lane = lax.broadcasted_iota(jnp.int32, (1, LANES), 1)
    for m in range(modules):
        factor = jnp.sum(jnp.where(at_lane == m, shrink, 0.0), axis=1, keepdims=True)
        clipped = grad[m] * factor
        moved = momentum_rate * momentum[m] + clipped
        new[m] = moved
        step[m] = (outer_rate * (clipped + momentum_rate * moved)).astype(jnp.bfloat16)
    for p in range(n):
        chosen[p] = step[module_ref[p]]
    for k in range(1, n):
        there, _ = peer(k)
        copy = pltpu.make_async_remote_copy(
            src_ref=chosen.at[there],
            dst_ref=update.at[0, :, block(me)],
            send_sem=back_send,
            recv_sem=back_recv,
            device_id=device(k),
            device_id_type=MESH,
        )
        copy.start()
    pltpu.make_async_copy(
        chosen.at[me], update.at[0, :, block(me)], back_recv
    ).start()
    arrived(pieces.at[pl.ds(0, n - 1)], send_sem)
    arrived(squares.at[pl.ds(0, len(everyone))], square_send)
    arrived(chosen.at[pl.ds(0, n - 1)], back_send)
    arrived(update, back_recv)


def write(update, new, update_ref, new_ref, sem):
    copies = [
        pltpu.make_async_copy(update, update_ref, sem.at[0]),
        pltpu.make_async_copy(new, new_ref, sem.at[1]),
    ]
    for copy in copies:
        copy.start()
    for copy in copies:
        copy.wait()


def direct(n, s, deltas, momentum, path_module):
    modules, rows, columns = momentum.shape
    width = deltas.shape[2]
    dma = pltpu.SemaphoreType.DMA
    anywhere = pl.BlockSpec(memory_space=pl.ANY)
    in_vmem = pl.BlockSpec(memory_space=pltpu.VMEM)
    held = pl.pallas_call(
        functools.partial(kernel, n, s),
        out_shape=(
            pltpu.VMEM(deltas.shape, jnp.bfloat16),
            pltpu.VMEM(momentum.shape, jnp.float32),
        ),
        in_specs=[anywhere, anywhere, anywhere],
        out_specs=(in_vmem, in_vmem),
        scratch_shapes=[
            pltpu.SMEM(path_module.shape, jnp.int32),
            pltpu.VMEM((rows, width), jnp.bfloat16),
            pltpu.VMEM((n, rows, columns), jnp.bfloat16),
            pltpu.VMEM((modules, rows, columns), jnp.float32),
            pltpu.VMEM((modules, rows, columns), jnp.float32),
            pltpu.VMEM((modules, rows, columns), jnp.bfloat16),
            pltpu.VMEM((n, rows, columns), jnp.bfloat16),
            pltpu.VMEM((1, LANES), jnp.float32),
            pltpu.VMEM((n * s, 1, LANES), jnp.float32),
            dma((3,)),
            dma,
            dma,
            dma,
            dma,
            dma,
            dma,
        ],
        compiler_params=pltpu.CompilerParams(collective_id=0, has_side_effects=True),
    )(deltas, momentum, path_module)
    return pl.pallas_call(
        write,
        out_shape=(
            jax.ShapeDtypeStruct(deltas.shape, jnp.bfloat16),
            jax.ShapeDtypeStruct(momentum.shape, jnp.float32),
        ),
        in_specs=[in_vmem, in_vmem],
        out_specs=(anywhere, anywhere),
        scratch_shapes=[dma((2,))],
    )(*[pltpu.with_memory_space_constraint(x, pltpu.VMEM) for x in held])


def by_collectives(s, deltas, momentum, path_module):
    modules = momentum.shape[0]
    rows, width = deltas.shape[1:]
    onehot = path_module[:, None] == jnp.arange(modules, dtype=jnp.int32)[None, :]
    counts = jnp.sum(onehot.astype(jnp.float32), axis=0)
    pieces = lax.all_to_all(deltas, "path", split_axis=2, concat_axis=0, tiled=True)
    totals = jnp.einsum(
        "pm,prc->mrc", onehot.astype(jnp.bfloat16), pieces, preferred_element_type=jnp.float32
    )
    outer_grad = totals / counts[:, None, None]
    local_squares = jnp.sum(outer_grad * outer_grad, axis=(1, 2))
    norm_squares = lax.psum(local_squares, ("path", "shard"))
    limit = clip_ratio * math.sqrt(rows * s * width)
    shrink = jnp.minimum(1.0, limit / jnp.sqrt(norm_squares + 1e-06))
    clipped = outer_grad * shrink[:, None, None]
    new_momentum = momentum_rate * momentum + clipped
    outer_step = (outer_rate * (clipped + momentum_rate * new_momentum)).astype(jnp.bfloat16)
    chosen = jnp.take(outer_step, path_module, axis=0)
    path_update = lax.all_to_all(chosen, "path", split_axis=0, concat_axis=2, tiled=True)
    return (path_update, new_momentum)


def local(n, s, deltas, momentum, path_module):
    modules, rows, columns = momentum.shape
    aligned = columns % LANES == 0 and rows % 16 == 0 and modules <= LANES
    if aligned and n > 1:
        return direct(n, s, deltas, momentum, path_module)
    return by_collectives(s, deltas, momentum, path_module)


def solution(mesh):
    return jax.shard_map(
        functools.partial(local, mesh.shape["path"], mesh.shape["shard"]),
        mesh=mesh,
        in_specs=(P("path", "shard", None), P(None, "shard", "path"), P()),
        out_specs=(P("path", "shard", None), P(None, "shard", "path")),
        check_vma=False,
    )
```

```python
import functools
import math

import jax
import jax.numpy as jnp
from jax import lax
from jax.experimental import pallas as pl
from jax.experimental.pallas import tpu as pltpu
from jax.sharding import PartitionSpec as P

outer_rate = 0.7
momentum_rate = 0.9
clip_ratio = 2.0
LANES = 128
MESH = pl.DeviceIdType.MESH


def kernel(
    n,
    s,
    deltas_ref,
    momentum_ref,
    path_module_ref,
    update,
    new,
    module_ref,
    own,
    pieces,
    momentum,
    grad,
    step,
    chosen,
    mine,
    squares,
    load_sem,
    send_sem,
    recv_sem,
    square_send,
    square_recv,
    back_send,
    back_recv,
):
    me, my_shard = lax.axis_index("path"), lax.axis_index("shard")
    modules, rows, columns = momentum.shape
    width = own.shape[1]
    everyone = [(k, j) for k in range(n) for j in range(s) if (k, j) != (0, 0)]

    def peer(k, j=0):
        there, shard = me + k, my_shard + j
        return jnp.where(there < n, there, there - n), jnp.where(shard < s, shard, shard - s)

    def device(k, j=0):
        there, shard = peer(k, j)
        return {"path": there, "shard": shard}

    def arrived(buffer, sem):
        pltpu.make_async_copy(buffer, buffer, sem).wait()

    def targets():
        size = math.gcd(n, 4)
        groups = n // size
        group, place = me // size, lax.rem(me, size)
        low = group < groups // 2
        for a in range(groups):
            down, up = groups - 1 - a, a
            down = jnp.where(down <= group, down - 1, down)
            up = jnp.where(up >= group, up + 1, up)
            other = group if a == groups - 1 else jnp.where(low, down, up)
            for b in range(1 if a == groups - 1 else 0, size):
                at = place + b
                yield other * size + jnp.where(at < size, at, at - size)

    def block(index):
        return pl.ds(pl.multiple_of(index * columns, columns), columns)

    barrier = pltpu.get_barrier_semaphore()
    for k, j in everyone:
        pl.semaphore_signal(barrier, inc=1, device_id=device(k, j), device_id_type=MESH)
    load_module = pltpu.make_async_copy(path_module_ref, module_ref, load_sem.at[2])
    load_module.start()
    load_own = pltpu.make_async_copy(deltas_ref.at[0], own, load_sem.at[0])
    load_own.start()
    load_momentum = pltpu.make_async_copy(momentum_ref, momentum, load_sem.at[1])
    load_momentum.start()
    load_module.wait()

    lane = lax.broadcasted_iota(jnp.int32, (1, n * rows), 1)
    target = jnp.zeros((1, n * rows), jnp.int32)
    for p in range(n):
        inside = (lane >= p * rows) & (lane < (p + 1) * rows)
        target = jnp.where(inside, lane + (module_ref[p] - p) * rows, target)
    row = lax.broadcasted_iota(jnp.int32, (modules * rows, n * rows), 0)
    spread = (row == target).astype(jnp.float32)
    scale = 1.0 / jnp.sum(spread, axis=1, keepdims=True)
    spread = spread.astype(jnp.bfloat16)

    load_own.wait()
    keep_own = pltpu.make_async_copy(own.at[:, block(me)], pieces.at[me], recv_sem)
    keep_own.start()
    pl.semaphore_wait(barrier, len(everyone))
    for there in targets():
        copy = pltpu.make_async_remote_copy(
            src_ref=own.at[:, block(there)],
            dst_ref=pieces.at[me],
            send_sem=send_sem,
            recv_sem=recv_sem,
            device_id={"path": there, "shard": my_shard},
            device_id_type=MESH,
        )
        copy.start()
    arrived(pieces, recv_sem)

    total = jnp.dot(
        spread, pieces[...].reshape(n * rows, columns), preferred_element_type=jnp.float32
    )
    outer_grad = (total * scale).reshape(modules, rows, columns)
    grad[...] = outer_grad
    by_row = jnp.sum(outer_grad * outer_grad, axis=1)
    by_module = jnp.sum(by_row, axis=1, keepdims=True)
    on_diagonal = lax.broadcasted_iota(
        jnp.int32, (modules, LANES), 0
    ) == lax.broadcasted_iota(jnp.int32, (modules, LANES), 1)
    own_squares = jnp.sum(jnp.where(on_diagonal, by_module, 0.0), axis=0, keepdims=True)
    my_slot = me * s + my_shard
    mine[...] = own_squares
    for k, j in everyone:
        copy = pltpu.make_async_remote_copy(
            src_ref=mine,
            dst_ref=squares.at[my_slot],
            send_sem=square_send,
            recv_sem=square_recv,
            device_id=device(k, j),
            device_id_type=MESH,
        )
        copy.start()
    pltpu.make_async_copy(mine, squares.at[my_slot], square_recv).start()
    load_momentum.wait()
    arrived(squares, square_recv)
    norm_squares = jnp.sum(squares[...], axis=0)
    limit = clip_ratio * math.sqrt(rows * s * width)
    shrink = jnp.minimum(1.0, limit / jnp.sqrt(norm_squares + 1e-06))
    at_lane = lax.broadcasted_iota(jnp.int32, (1, LANES), 1)
    for m in range(modules):
        factor = jnp.sum(jnp.where(at_lane == m, shrink, 0.0), axis=1, keepdims=True)
        clipped = grad[m] * factor
        moved = momentum_rate * momentum[m] + clipped
        new[m] = moved
        step[m] = (outer_rate * (clipped + momentum_rate * moved)).astype(jnp.bfloat16)
    chosen[me] = step[module_ref[me]]
    for k in range(1, n):
        there, _ = peer(k)
        chosen[there] = step[module_ref[there]]
        copy = pltpu.make_async_remote_copy(
            src_ref=chosen.at[there],
            dst_ref=update.at[0, :, block(me)],
            send_sem=back_send,
            recv_sem=back_recv,
            device_id=device(k),
            device_id_type=MESH,
        )
        copy.start()
    pltpu.make_async_copy(
        chosen.at[me], update.at[0, :, block(me)], back_recv
    ).start()
    arrived(pieces.at[pl.ds(0, n - 1)], send_sem)
    arrived(squares.at[pl.ds(0, len(everyone))], square_send)
    arrived(chosen.at[pl.ds(0, n - 1)], back_send)
    arrived(update, back_recv)


def write(update, new, update_ref, new_ref, sem):
    copies = [
        pltpu.make_async_copy(update, update_ref, sem.at[0]),
        pltpu.make_async_copy(new, new_ref, sem.at[1]),
    ]
    for copy in copies:
        copy.start()
    for copy in copies:
        copy.wait()


def direct(n, s, deltas, momentum, path_module):
    modules, rows, columns = momentum.shape
    width = deltas.shape[2]
    dma = pltpu.SemaphoreType.DMA
    anywhere = pl.BlockSpec(memory_space=pl.ANY)
    in_vmem = pl.BlockSpec(memory_space=pltpu.VMEM)
    held = pl.pallas_call(
        functools.partial(kernel, n, s),
        out_shape=(
            pltpu.VMEM(deltas.shape, jnp.bfloat16),
            pltpu.VMEM(momentum.shape, jnp.float32),
        ),
        in_specs=[anywhere, anywhere, anywhere],
        out_specs=(in_vmem, in_vmem),
        scratch_shapes=[
            pltpu.SMEM(path_module.shape, jnp.int32),
            pltpu.VMEM((rows, width), jnp.bfloat16),
            pltpu.VMEM((n, rows, columns), jnp.bfloat16),
            pltpu.VMEM((modules, rows, columns), jnp.float32),
            pltpu.VMEM((modules, rows, columns), jnp.float32),
            pltpu.VMEM((modules, rows, columns), jnp.bfloat16),
            pltpu.VMEM((n, rows, columns), jnp.bfloat16),
            pltpu.VMEM((1, LANES), jnp.float32),
            pltpu.VMEM((n * s, 1, LANES), jnp.float32),
            dma((3,)),
            dma,
            dma,
            dma,
            dma,
            dma,
            dma,
        ],
        compiler_params=pltpu.CompilerParams(collective_id=0, has_side_effects=True),
    )(deltas, momentum, path_module)
    return pl.pallas_call(
        write,
        out_shape=(
            jax.ShapeDtypeStruct(deltas.shape, jnp.bfloat16),
            jax.ShapeDtypeStruct(momentum.shape, jnp.float32),
        ),
        in_specs=[in_vmem, in_vmem],
        out_specs=(anywhere, anywhere),
        scratch_shapes=[dma((2,))],
    )(*[pltpu.with_memory_space_constraint(x, pltpu.VMEM) for x in held])


def by_collectives(s, deltas, momentum, path_module):
    modules = momentum.shape[0]
    rows, width = deltas.shape[1:]
    onehot = path_module[:, None] == jnp.arange(modules, dtype=jnp.int32)[None, :]
    counts = jnp.sum(onehot.astype(jnp.float32), axis=0)
    pieces = lax.all_to_all(deltas, "path", split_axis=2, concat_axis=0, tiled=True)
    totals = jnp.einsum(
        "pm,prc->mrc", onehot.astype(jnp.bfloat16), pieces, preferred_element_type=jnp.float32
    )
    outer_grad = totals / counts[:, None, None]
    local_squares = jnp.sum(outer_grad * outer_grad, axis=(1, 2))
    norm_squares = lax.psum(local_squares, ("path", "shard"))
    limit = clip_ratio * math.sqrt(rows * s * width)
    shrink = jnp.minimum(1.0, limit / jnp.sqrt(norm_squares + 1e-06))
    clipped = outer_grad * shrink[:, None, None]
    new_momentum = momentum_rate * momentum + clipped
    outer_step = (outer_rate * (clipped + momentum_rate * new_momentum)).astype(jnp.bfloat16)
    chosen = jnp.take(outer_step, path_module, axis=0)
    path_update = lax.all_to_all(chosen, "path", split_axis=0, concat_axis=2, tiled=True)
    return (path_update, new_momentum)


def local(n, s, deltas, momentum, path_module):
    modules, rows, columns = momentum.shape
    aligned = columns % LANES == 0 and rows % 16 == 0 and modules <= LANES
    if aligned and n > 1:
        return direct(n, s, deltas, momentum, path_module)
    return by_collectives(s, deltas, momentum, path_module)


def solution(mesh):
    return jax.shard_map(
        functools.partial(local, mesh.shape["path"], mesh.shape["shard"]),
        mesh=mesh,
        in_specs=(P("path", "shard", None), P(None, "shard", "path"), P()),
        out_specs=(P("path", "shard", None), P(None, "shard", "path")),
        check_vma=False,
    )
```
